32 devices in a mesh: lat: 8 (over y, x, core), depth: 4 (over z).
Axes of the slice: x: 2, y: 2, z: 4, core: 2. Of those that a mesh axis runs over, the one named last changes fastest.
Arguments:
- velocity_fine: float32 [3, 96, 64, 384], P(None, 'lat', 'depth'), may hold values from -6 to 6
- stress_fine: float32 [6, 96, 64, 384], P(None, 'lat', 'depth'), may hold values from -6 to 6
- memory_fine: float32 [6, 96, 64, 384], P(None, 'lat', 'depth'), may hold values from -1.8 to 1.8
- peak_fine: float32 [96, 64, 384], P('lat', 'depth'), may hold values from 0 to 12
- zone_fine: int32 [96, 64, 384], P('lat', 'depth'), may hold values from 0 to 7
- velocity_coarse: float32 [3, 32, 128, 128], P(None, 'lat', 'depth'), may hold values from -6 to 6
- stress_coarse: float32 [6, 32, 128, 128], P(None, 'lat', 'depth'), may hold values from -6 to 6
- memory_coarse: float32 [6, 32, 128, 128], P(None, 'lat', 'depth'), may hold values from -1.8 to 1.8
- peak_coarse: float32 [32, 128, 128], P('lat', 'depth'), may hold values from 0 to 12
- zone_coarse: int32 [32, 128, 128], P('lat', 'depth'), may hold values from 0 to 7
- zone_table: float32 [8, 5], replicated, may hold values from 0.05 to 1, as said below
- interp_weight: int32 [2, 3], replicated, may hold values from 0 to 8
- restrict_weight: int32 [2, 3], replicated, may hold values from 1 to 8
Outputs:
- fine_velocity: float32 [3, 96, 64, 384], P(None, 'lat', 'depth')
- fine_stress: float32 [6, 96, 64, 384], P(None, 'lat', 'depth')
- fine_memory: float32 [6, 96, 64, 384], P(None, 'lat', 'depth')
- fine_peak: float32 [96, 64, 384], P('lat', 'depth')
- coarse_velocity: float32 [3, 32, 128, 128], P(None, 'lat', 'depth')
- coarse_stress: float32 [6, 32, 128, 128], P(None, 'lat', 'depth')
- coarse_memory: float32 [6, 32, 128, 128], P(None, 'lat', 'depth')
- coarse_peak: float32 [32, 128, 128], P('lat', 'depth')
The draws below stay inside these ranges and needn't reach their ends.
Inputs may be any that keep to these rules, and one draw needn't show every extreme that they name: `zone_table`: column 0 lies in 0.5 to 1, columns 1 and 2 in 0.1 to 0.3, column 3 in 0.5 to 0.95, column 4 in 0.05 to 0.3.
All inputs are finite; a program needn't handle non-finite values.
Results may differ from the reference program's by a relative error of at most 0.0003.
Values sent between devices are 32-bit elements; how exact they have to be, the bound alone decides.
A program may use at most 128 MiB of HBM per device.

```python
import jax
import jax.numpy as jnp
from jax import lax

NYC = 128
ZONES = 8
STEPS = 2
NYF = 384
NXC = 32
NXF = 96
NZF = 64
NZC = 128


def draw_zone_table(key, part):
    lower_edge = jnp.array([0.5, 0.1, 0.1, 0.5, 0.05], jnp.float32)
    upper_edge = jnp.array([1.0, 0.3, 0.3, 0.95, 0.3], jnp.float32)
    unit = jax.random.uniform(jax.random.fold_in(key, 17), (ZONES, 5), jnp.float32)
    return lower_edge + (upper_edge - lower_edge) * unit


def with_ends(values, rng, least, largest):
    extent = values.shape
    spot = [jax.random.randint(jax.random.fold_in(rng, axis), (), 0, extent[axis]) for axis in range(len(extent))]
    values = values.at[tuple(spot)].set(least)
    longest = extent.index(max(extent))
    spot[longest] = (spot[longest] + 1) % extent[longest]
    return values.at[tuple(spot)].set(largest)


def levels(stream_key, shape, pieces, low, high):
    factor_of, own = 1.0, jax.random.fold_in(stream_key, 6)
    for dim, blocks in pieces:
        draws = jnp.exp(jax.random.uniform(jax.random.fold_in(own, dim), (blocks,), jnp.float32, low / len(pieces), high / len(pieces)))
        factor_of = factor_of * jnp.repeat(draws, shape[dim] // blocks).reshape([-1 if axis == dim else 1 for axis in range(len(shape))])
    return factor_of


def noise(key, dims, scale, limit, cuts=(), kind=jnp.bfloat16):
    drawn = jax.random.normal(key, dims, jnp.float32) * scale
    if len(cuts) > 0:
        drawn = levels(key, dims, cuts, -0.22, 0.18) * drawn
    return jnp.clip(drawn, min=-limit, max=limit).astype(kind)


def setup_inputs(seed: int = 0) -> dict:
    seeds = jax.random.split(jax.random.key(seed), 14)
    return {
        "velocity_fine": noise(seeds[0], (3, NXF, NZF, NYF), 1.0, 6.0, ((1, 8), (2, 4)), jnp.float32),
        "stress_fine": noise(seeds[1], (6, NXF, NZF, NYF), 1.0, 6.0, ((1, 8), (2, 4)), jnp.float32),
        "memory_fine": noise(seeds[2], (6, NXF, NZF, NYF), 0.3, 1.8, ((1, 8), (2, 4)), jnp.float32),
        "peak_fine": jnp.clip(12.0 * jax.random.uniform(seeds[3], (NXF, NZF, NYF), jnp.float32) ** levels(seeds[3], (NXF, NZF, NYF), ((0, 8), (1, 4)), -0.2, 0.2), 0.0, 12.0),
        "zone_fine": with_ends(jax.random.randint(seeds[4], (NXF, NZF, NYF), 0, ZONES), jax.random.fold_in(seeds[4], 1), 0, ZONES - 1).astype(jnp.int32),
        "velocity_coarse": noise(seeds[5], (3, NXC, NZC, NYC), 1.0, 6.0, ((1, 8), (2, 4)), jnp.float32),
        "stress_coarse": noise(seeds[6], (6, NXC, NZC, NYC), 1.0, 6.0, ((1, 8), (2, 4)), jnp.float32),
        "memory_coarse": noise(seeds[7], (6, NXC, NZC, NYC), 0.3, 1.8, ((1, 8), (2, 4)), jnp.float32),
        "peak_coarse": jnp.clip(12.0 * jax.random.uniform(seeds[8], (NXC, NZC, NYC), jnp.float32) ** levels(seeds[8], (NXC, NZC, NYC), ((0, 8), (1, 4)), -0.2, 0.2), 0.0, 12.0),
        "zone_coarse": with_ends(jax.random.randint(seeds[9], (NXC, NZC, NYC), 0, ZONES), jax.random.fold_in(seeds[9], 1), 0, ZONES - 1).astype(jnp.int32),
        "zone_table": draw_zone_table(jax.random.fold_in(seeds[13], 71), 0),
        "interp_weight": with_ends(jax.random.randint(seeds[11], (2, 3), 0, 9), jax.random.fold_in(seeds[11], 1), 0, 8).astype(jnp.int32),
        "restrict_weight": with_ends(jax.random.randint(seeds[12], (2, 3), 1, 9), jax.random.fold_in(seeds[12], 1), 1, 8).astype(jnp.int32),
    }


time_step = 0.4
near_coef = 9.0 / 8.0
far_coef = 1.0 / 24.0

def shifted(field, axis, offset):
    index = [slice(None), slice(2, -2), slice(2, -2), slice(2, -2)]
    index[axis] = slice(2 + offset, field.shape[axis] - 2 + offset)
    return field[tuple(index)]

def forward(field, axis):
    return near_coef * (shifted(field, axis, 1) - shifted(field, axis, 0)) - far_coef * (shifted(field, axis, 2) - shifted(field, axis, -1))

def backward(field, axis):
    return near_coef * (shifted(field, axis, 0) - shifted(field, axis, -1)) - far_coef * (shifted(field, axis, 1) - shifted(field, axis, -2))

def materials(zone, zone_table):
    columns = []
    for column in range(5):
        value = jnp.zeros(zone.shape, jnp.float32)
        for level in range(zone_table.shape[0]):
            value = jnp.where(zone == level, zone_table[level, column], value)
        columns.append(value)
    return columns

def velocity_update(padded, velocity, buoyancy, spacing):

    def part(index):
        return padded[index:index + 1]
    accel_x = forward(part(0), 1) + backward(part(3), 3) + backward(part(4), 2)
    accel_y = backward(part(3), 1) + forward(part(1), 3) + backward(part(5), 2)
    accel_z = backward(part(4), 1) + backward(part(5), 3) + forward(part(2), 2)
    accel = jnp.concatenate([accel_x, accel_y, accel_z], axis=0)
    return velocity + time_step / spacing * buoyancy[None] * accel

def stress_update(padded, stress, memory, props, spacing):
    lame, shear, decay, damping = (props[1][None], props[2][None], props[3][None], props[4][None])

    def part(index):
        return padded[index:index + 1]
    normal_x = backward(part(0), 1)
    normal_y = backward(part(1), 3)
    normal_z = backward(part(2), 2)
    shear_xy = 0.5 * (forward(part(0), 3) + forward(part(1), 1))
    shear_xz = 0.5 * (forward(part(0), 2) + forward(part(2), 1))
    shear_yz = 0.5 * (forward(part(1), 2) + forward(part(2), 3))
    volume = normal_x + normal_y + normal_z
    rate = jnp.concatenate([lame * volume + 2.0 * shear * normal_x, lame * volume + 2.0 * shear * normal_y, lame * volume + 2.0 * shear * normal_z, 2.0 * shear * shear_xy, 2.0 * shear * shear_xz, 2.0 * shear * shear_yz], axis=0) / spacing
    memory_next = decay * memory - damping * (1.0 - decay) * rate
    stress_next = stress + time_step * (rate + 0.5 * (memory + memory_next))
    return (stress_next, memory_next)

def entry_key(first, second):
    return (min(first, second), max(first, second))

def rotate(entries, first, second):
    other = 3 - first - second
    pivot = entries[first, second]
    gap = entries[second, second] - entries[first, first]
    denominator = jnp.abs(gap) + jnp.sqrt(gap * gap + 4.0 * pivot * pivot)
    direction = jnp.where(gap >= 0, 1.0, -1.0)
    usable = denominator > 0
    tangent = jnp.where(usable, 2.0 * pivot * direction / jnp.where(usable, denominator, 1.0), 0.0)
    cosine = 1.0 / jnp.sqrt(1.0 + tangent * tangent)
    sine = tangent * cosine
    low_entry = entries[entry_key(other, first)]
    high_entry = entries[entry_key(other, second)]
    result = dict(entries)
    result[first, first] = entries[first, first] - tangent * pivot
    result[second, second] = entries[second, second] + tangent * pivot
    result[first, second] = jnp.zeros_like(pivot)
    result[entry_key(other, first)] = cosine * low_entry - sine * high_entry
    result[entry_key(other, second)] = sine * low_entry + cosine * high_entry
    return result

def strain_peak(stress, props, peak):
    lame, shear = (props[1], props[2])
    trace = stress[0] + stress[1] + stress[2]
    isotropic = lame * trace / (3.0 * lame + 2.0 * shear)
    scale = 0.5 / shear
    entries = {(0, 0): (stress[0] - isotropic) * scale, (1, 1): (stress[1] - isotropic) * scale, (2, 2): (stress[2] - isotropic) * scale, (0, 1): stress[3] * scale, (0, 2): stress[4] * scale, (1, 2): stress[5] * scale}
    for sweep in range(3):
        entries = rotate(entries, 0, 1)
        entries = rotate(entries, 0, 2)
        entries = rotate(entries, 1, 2)
    principal = jnp.maximum(jnp.maximum(entries[0, 0], entries[1, 1]), entries[2, 2])
    return jnp.maximum(peak, principal)

def make_tables(interp_weight, restrict_weight, coarse_cells):
    x_share = interp_weight[0].astype(jnp.float32) / 8.0
    y_share = interp_weight[1].astype(jnp.float32) / 8.0
    x_weight = restrict_weight[0].astype(jnp.float32)
    y_weight = restrict_weight[1].astype(jnp.float32)
    coarse_index = lax.broadcasted_iota(jnp.int32, (coarse_cells, 3 * coarse_cells), 0)
    fine_index = lax.broadcasted_iota(jnp.int32, (coarse_cells, 3 * coarse_cells), 1)
    phase = fine_index % 3
    block = fine_index // 3
    y_interp = jnp.where(phase == 0, y_share[0], jnp.where(phase == 1, y_share[1], y_share[2]))
    y_restrict = jnp.where(phase == 0, y_weight[0], jnp.where(phase == 1, y_weight[1], y_weight[2]))
    y_spread = jnp.where(coarse_index == block, y_interp, 0.0) + jnp.where(coarse_index == block + 1, 1.0 - y_interp, 0.0)
    y_gather = jnp.where(coarse_index == block, y_restrict, 0.0).T
    normaliser = 3.0 * jnp.sum(x_weight) * jnp.sum(y_weight)
    return (x_share, y_spread, x_weight, y_gather, normaliser)

def interpolate(planes, tables):
    x_share, y_spread = (tables[0], tables[1])
    upper = planes[:, :, 0:1]
    lower = planes[:, :, 1:2]
    layered = jnp.concatenate([(2.0 * upper + lower) / 3.0, (upper + 2.0 * lower) / 3.0], axis=2)
    share = x_share[None, None, :, None, None]
    across = share * layered[:, :-1, None] + (1.0 - share) * layered[:, 1:, None]
    count, rows = (across.shape[0], across.shape[1])
    flat = across.reshape(count * rows * 6, -1)
    spread = jnp.dot(flat, y_spread, precision=lax.Precision.HIGHEST)
    return spread.reshape(count, rows * 3, 2, -1)

def restrict(block, tables):
    x_weight, y_gather, normaliser = (tables[2], tables[3], tables[4])
    count, rows = (block.shape[0], block.shape[1])
    layers = lax.optimization_barrier(jnp.sum(block.reshape(count, rows, 2, 3, -1), axis=3))
    grouped = layers.reshape(count, rows // 3, 3, 2, -1)
    across = lax.optimization_barrier(jnp.sum(x_weight[None, None, :, None, None] * grouped, axis=2))
    flat = across.reshape(count * (rows // 3) * 2, -1)
    gathered = jnp.dot(flat, y_gather, precision=lax.Precision.HIGHEST)
    return gathered.reshape(count, rows // 3, 2, -1) / normaliser

def pad_fine(fine, coarse, tables):
    planes = jnp.pad(coarse[:, :, 0:2], ((0, 0), (0, 1), (0, 0), (0, 0)))
    ghost = interpolate(planes, tables)
    column = jnp.concatenate([jnp.zeros_like(fine[:, :, 0:2]), fine, ghost], axis=2)
    return jnp.pad(column, ((0, 0), (2, 2), (0, 0), (2, 2)))

def pad_coarse(coarse, fine, tables):
    ghost = restrict(fine[:, :, -6:], tables)
    column = jnp.concatenate([ghost, coarse, jnp.zeros_like(coarse[:, :, 0:2])], axis=2)
    return jnp.pad(column, ((0, 0), (2, 2), (0, 0), (2, 2)))

def reference(velocity_fine, stress_fine, memory_fine, peak_fine, zone_fine, velocity_coarse, stress_coarse, memory_coarse, peak_coarse, zone_coarse, zone_table, interp_weight, restrict_weight):
    tables = make_tables(interp_weight, restrict_weight, stress_coarse.shape[3])
    props_fine = materials(zone_fine, zone_table)
    props_coarse = materials(zone_coarse, zone_table)
    for step in range(STEPS):
        padded_fine = pad_fine(stress_fine, stress_coarse, tables)
        padded_coarse = pad_coarse(stress_coarse, stress_fine, tables)
        velocity_fine = velocity_update(padded_fine, velocity_fine, props_fine[0], 1.0)
        velocity_coarse = velocity_update(padded_coarse, velocity_coarse, props_coarse[0], 3.0)
        padded_fine = pad_fine(velocity_fine, velocity_coarse, tables)
        padded_coarse = pad_coarse(velocity_coarse, velocity_fine, tables)
        stress_fine, memory_fine = stress_update(padded_fine, stress_fine, memory_fine, props_fine, 1.0)
        stress_coarse, memory_coarse = stress_update(padded_coarse, stress_coarse, memory_coarse, props_coarse, 3.0)
        peak_fine = strain_peak(stress_fine, props_fine, peak_fine)
        peak_coarse = strain_peak(stress_coarse, props_coarse, peak_coarse)
    return (velocity_fine, stress_fine, memory_fine, peak_fine, velocity_coarse, stress_coarse, memory_coarse, peak_coarse)
```

```python
import jax
import jax.numpy as jnp
from jax import lax
from jax.experimental import pallas as pl
from jax.experimental.pallas import tpu as pltpu
from jax.sharding import PartitionSpec as P

STEPS = 2


time_step = 0.4
near_coef = 9.0 / 8.0
far_coef = 1.0 / 24.0


def derivative(field, low, high, dim):
    wide = jnp.concatenate([low, field, high], axis=dim)
    count = field.shape[dim]

    def at(begin):
        return lax.slice_in_dim(wide, begin, begin + count, axis=dim)

    return near_coef * (at(2) - at(1)) - far_coef * (at(3) - at(0))


FORWARD = (1, 2)
BACKWARD = (2, 1)


def derivative_y(field, kind):
    wide = jnp.pad(field, ((0, 0), (0, 0), kind))
    count = field.shape[2]

    def at(begin):
        return lax.slice_in_dim(wide, begin, begin + count, axis=2)

    return near_coef * (at(2) - at(1)) - far_coef * (at(3) - at(0))


def materials_kernel(table_ref, zone_ref, *column_refs):

    def row(index, carry):
        zone = zone_ref[index]
        masks = [zone == level for level in range(1, table_ref.shape[0])]
        for column, ref in enumerate(column_refs):
            value = jnp.full(zone.shape, table_ref[0, column], jnp.float32)
            for level, mask in enumerate(masks):
                value = jnp.where(mask, table_ref[level + 1, column], value)
            ref[index] = value
        return carry

    lax.fori_loop(0, zone_ref.shape[0], row, 0)


def materials(zone, zone_table):
    whole = pl.BlockSpec(memory_space=pltpu.VMEM)
    return pl.pallas_call(
        materials_kernel,
        out_shape=[jax.ShapeDtypeStruct(zone.shape, jnp.float32)] * 5,
        in_specs=[pl.BlockSpec(memory_space=pltpu.SMEM), whole],
        out_specs=[whole] * 5,
    )(zone_table, zone)


STRESS_X = ((0, FORWARD), (3, BACKWARD), (4, BACKWARD))
STRESS_Z = ((4, BACKWARD), (5, BACKWARD), (2, FORWARD))
VELOCITY_X = ((0, BACKWARD), (1, FORWARD), (2, FORWARD))
VELOCITY_Z = ((0, FORWARD), (1, FORWARD), (2, BACKWARD))


def velocity_update(stress, velocity, buoyancy, spacing, ghosts):
    low_x, high_x, low_z, high_z = ghosts

    def along_x(slot):
        return derivative(stress[STRESS_X[slot][0]], low_x[slot], high_x[slot], 0)

    def along_z(slot):
        return derivative(stress[STRESS_Z[slot][0]], low_z[slot], high_z[slot], 1)

    accel_x = along_x(0) + derivative_y(stress[3], BACKWARD) + along_z(0)
    accel_y = along_x(1) + derivative_y(stress[1], FORWARD) + along_z(1)
    accel_z = along_x(2) + derivative_y(stress[5], BACKWARD) + along_z(2)
    accel = jnp.stack([accel_x, accel_y, accel_z])
    return velocity + time_step / spacing * buoyancy[None] * accel


def stress_update(velocity, stress, memory, props, spacing, ghosts):
    lame, shear, decay, damping = props[1:]
    low_x, high_x, low_z, high_z = ghosts

    def along_x(part):
        return derivative(velocity[part], low_x[part], high_x[part], 0)

    def along_z(part):
        return derivative(velocity[part], low_z[part], high_z[part], 1)

    normal_x = along_x(0)
    normal_y = derivative_y(velocity[1], BACKWARD)
    normal_z = along_z(2)
    shear_xy = 0.5 * (derivative_y(velocity[0], FORWARD) + along_x(1))
    shear_xz = 0.5 * (along_z(0) + along_x(2))
    shear_yz = 0.5 * (along_z(1) + derivative_y(velocity[2], FORWARD))
    volume = normal_x + normal_y + normal_z
    rate = (
        jnp.stack(
            [
                lame * volume + 2.0 * shear * normal_x,
                lame * volume + 2.0 * shear * normal_y,
                lame * volume + 2.0 * shear * normal_z,
                2.0 * shear * shear_xy,
                2.0 * shear * shear_xz,
                2.0 * shear * shear_yz,
            ]
        )
        / spacing
    )
    memory_next = decay[None] * memory - (damping * (1.0 - decay))[None] * rate
    stress_next = stress + time_step * (rate + 0.5 * (memory + memory_next))
    return (stress_next, memory_next)


def entry_key(first, second):
    return (min(first, second), max(first, second))


def rotate(entries, first, second):
    other = 3 - first - second
    pivot = entries[first, second]
    gap = entries[second, second] - entries[first, first]
    denominator = jnp.abs(gap) + jnp.sqrt(gap * gap + 4.0 * pivot * pivot)
    direction = jnp.where(gap >= 0, 1.0, -1.0)
    usable = denominator > 0
    tangent = jnp.where(usable, 2.0 * pivot * direction / jnp.where(usable, denominator, 1.0), 0.0)
    cosine = 1.0 / jnp.sqrt(1.0 + tangent * tangent)
    sine = tangent * cosine
    low_entry = entries[entry_key(other, first)]
    high_entry = entries[entry_key(other, second)]
    result = dict(entries)
    result[first, first] = entries[first, first] - tangent * pivot
    result[second, second] = entries[second, second] + tangent * pivot
    result[first, second] = jnp.zeros_like(pivot)
    result[entry_key(other, first)] = cosine * low_entry - sine * high_entry
    result[entry_key(other, second)] = sine * low_entry + cosine * high_entry
    return result


def strain_peak(stress, props, peak):
    lame, shear = (props[1], props[2])
    trace = stress[0] + stress[1] + stress[2]
    isotropic = lame * trace / (3.0 * lame + 2.0 * shear)
    scale = 0.5 / shear
    entries = {
        (0, 0): (stress[0] - isotropic) * scale,
        (1, 1): (stress[1] - isotropic) * scale,
        (2, 2): (stress[2] - isotropic) * scale,
        (0, 1): stress[3] * scale,
        (0, 2): stress[4] * scale,
        (1, 2): stress[5] * scale,
    }
    for sweep in range(3):
        entries = rotate(entries, 0, 1)
        entries = rotate(entries, 0, 2)
        entries = rotate(entries, 1, 2)
    principal = jnp.maximum(jnp.maximum(entries[0, 0], entries[1, 1]), entries[2, 2])
    return jnp.maximum(peak, principal)


def make_tables(interp_weight, restrict_weight, coarse_cells):
    x_share = interp_weight[0].astype(jnp.float32) / 8.0
    y_share = interp_weight[1].astype(jnp.float32) / 8.0
    x_weight = restrict_weight[0].astype(jnp.float32)
    y_weight = restrict_weight[1].astype(jnp.float32)
    coarse_index = lax.broadcasted_iota(jnp.int32, (coarse_cells, 3 * coarse_cells), 0)
    fine_index = lax.broadcasted_iota(jnp.int32, (coarse_cells, 3 * coarse_cells), 1)
    phase = fine_index % 3
    block = fine_index // 3
    y_interp = jnp.where(phase == 0, y_share[0], jnp.where(phase == 1, y_share[1], y_share[2]))
    y_restrict = jnp.where(phase == 0, y_weight[0], jnp.where(phase == 1, y_weight[1], y_weight[2]))
    y_spread = jnp.where(coarse_index == block, y_interp, 0.0) + jnp.where(
        coarse_index == block + 1, 1.0 - y_interp, 0.0
    )
    y_gather = jnp.where(coarse_index == block, y_restrict, 0.0).T
    normaliser = 3.0 * jnp.sum(x_weight) * jnp.sum(y_weight)
    return (x_share, y_spread, x_weight, y_gather, normaliser)


def interpolate(planes, tables):
    x_share, y_spread = (tables[0], tables[1])
    upper = planes[:, :, 0:1]
    lower = planes[:, :, 1:2]
    layered = jnp.concatenate([(2.0 * upper + lower) / 3.0, (upper + 2.0 * lower) / 3.0], axis=2)
    share = x_share[None, None, :, None, None]
    across = share * layered[:, :-1, None] + (1.0 - share) * layered[:, 1:, None]
    count, rows = (across.shape[0], across.shape[1])
    flat = across.reshape(count * rows * 6, -1)
    spread = jnp.dot(flat, y_spread, precision=lax.Precision.HIGHEST)
    return spread.reshape(count, rows * 3, 2, -1)


def restrict(block, tables):
    x_weight, y_gather, normaliser = (tables[2], tables[3], tables[4])
    count, rows = (block.shape[0], block.shape[1])
    layers = jnp.sum(block.reshape(count, rows, 2, 3, -1), axis=3)
    grouped = layers.reshape(count, rows // 3, 3, 2, -1)
    across = jnp.sum(x_weight[None, None, :, None, None] * grouped, axis=2)
    flat = across.reshape(count * (rows // 3) * 2, -1)
    gathered = jnp.dot(flat, y_gather, precision=lax.Precision.HIGHEST)
    return gathered.reshape(count, rows // 3, 2, -1) / normaliser


def lane_slabs(block, width, dim):
    count = block.shape[-1] // width
    slabs = [block[..., i * width : (i + 1) * width] for i in range(count)]
    return jnp.concatenate(slabs, axis=dim)


def lane_joined(block, count, dim):
    return jnp.concatenate(jnp.split(block, count, axis=dim), axis=-1)


def lateral_message(fine, coarse):
    folds = coarse.shape[1] // fine.shape[1]
    return jnp.concatenate([fine, lane_joined(coarse, folds, 1)], axis=-1)


def cut_rows(block, kinds, side):
    parts = []
    begin = 0
    for _, kind in kinds:
        parts.append(block[begin : begin + kind[side]])
        begin += kind[side]
    return parts


def exchange(fine, coarse, along_x, along_z, tables):
    lats = lax.axis_size("lat")
    depths = lax.axis_size("depth")
    depth_index = lax.axis_index("depth")

    def low_rows(field):
        return jnp.concatenate([field[part, -kind[0] :] for part, kind in along_x], axis=0)

    def high_rows(field):
        return jnp.concatenate([field[part, : kind[1]] for part, kind in along_x], axis=0)

    def layers(field, begin, end):
        return jnp.stack([field[part, :, begin:end] for part, _ in along_z])

    from_below = lax.ppermute(
        lateral_message(low_rows(fine), low_rows(coarse)),
        "lat",
        [(i, i + 1) for i in range(lats - 1)],
    )
    from_above = lax.ppermute(
        lateral_message(high_rows(fine), high_rows(coarse)),
        "lat",
        [(i + 1, i) for i in range(lats - 1)],
    )
    width = coarse.shape[3]
    folds = fine.shape[3] // width
    split = fine.shape[1] * folds
    coarse_head = layers(coarse, 0, 2)
    head = jnp.concatenate([lane_slabs(layers(fine, 0, 2), width, 1), coarse_head], axis=1)
    from_next = lax.ppermute(head, "depth", [((i + 1) % depths, i) for i in range(depths)])
    corner = lax.ppermute(
        coarse_head[:, :1],
        ("lat", "depth"),
        [((i + 1) * depths, i * depths + depths - 1) for i in range(lats - 1)],
    )
    size = fine.shape[2]
    lifted = restrict(layers(fine, size - 6, size), tables)
    deep = coarse.shape[2]
    coarse_tail = jnp.where(depth_index == depths - 1, lifted, layers(coarse, deep - 2, deep))
    tail = jnp.concatenate(
        [lane_slabs(layers(fine, size - 2, size), width, 1), coarse_tail], axis=1
    )
    from_previous = lax.ppermute(tail, "depth", [(i, (i + 1) % depths) for i in range(depths)])

    fine_below, coarse_below = (
        from_below[..., : fine.shape[3]],
        lane_slabs(from_below[..., fine.shape[3] :], width, 1),
    )
    fine_above, coarse_above = (
        from_above[..., : fine.shape[3]],
        lane_slabs(from_above[..., fine.shape[3] :], width, 1),
    )
    fine_low = jnp.where(depth_index == 0, 0.0, lane_joined(from_previous[:, :split], folds, 1))
    coarse_low = from_previous[:, split:]
    received = from_next[:, split:]
    ghost = interpolate(jnp.concatenate([received, corner], axis=1), tables)
    last = depth_index == depths - 1
    fine_high = jnp.where(last, ghost, lane_joined(from_next[:, :split], folds, 1))
    coarse_high = jnp.where(last, 0.0, received)

    def ghosts(below, above, low, high):
        return (
            cut_rows(below, along_x, 0),
            cut_rows(above, along_x, 1),
            [low[slot, :, 2 - kind[0] :] for slot, (_, kind) in enumerate(along_z)],
            [high[slot, :, : kind[1]] for slot, (_, kind) in enumerate(along_z)],
        )

    return (
        ghosts(fine_below, fine_above, fine_low, fine_high),
        ghosts(coarse_below, coarse_above, coarse_low, coarse_high),
    )


def on_device(
    velocity_fine,
    stress_fine,
    memory_fine,
    peak_fine,
    zone_fine,
    velocity_coarse,
    stress_coarse,
    memory_coarse,
    peak_coarse,
    zone_coarse,
    zone_table,
    interp_weight,
    restrict_weight,
):
    tables = make_tables(interp_weight, restrict_weight, stress_coarse.shape[3])
    props_fine = materials(zone_fine, zone_table)
    props_coarse = materials(zone_coarse, zone_table)
    for step in range(STEPS):
        fine_ghosts, coarse_ghosts = exchange(
            stress_fine, stress_coarse, STRESS_X, STRESS_Z, tables
        )
        velocity_fine = velocity_update(
            stress_fine, velocity_fine, props_fine[0], 1.0, fine_ghosts
        )
        velocity_coarse = velocity_update(
            stress_coarse, velocity_coarse, props_coarse[0], 3.0, coarse_ghosts
        )
        fine_ghosts, coarse_ghosts = exchange(
            velocity_fine, velocity_coarse, VELOCITY_X, VELOCITY_Z, tables
        )
        stress_fine, memory_fine = stress_update(
            velocity_fine, stress_fine, memory_fine, props_fine, 1.0, fine_ghosts
        )
        stress_coarse, memory_coarse = stress_update(
            velocity_coarse, stress_coarse, memory_coarse, props_coarse, 3.0, coarse_ghosts
        )
        peak_fine = strain_peak(stress_fine, props_fine, peak_fine)
        peak_coarse = strain_peak(stress_coarse, props_coarse, peak_coarse)
    return (
        velocity_fine,
        stress_fine,
        memory_fine,
        peak_fine,
        velocity_coarse,
        stress_coarse,
        memory_coarse,
        peak_coarse,
    )


def solution(mesh):
    in_specs = (
        P(None, "lat", "depth", None),
        P(None, "lat", "depth", None),
        P(None, "lat", "depth", None),
        P("lat", "depth", None),
        P("lat", "depth", None),
        P(None, "lat", "depth", None),
        P(None, "lat", "depth", None),
        P(None, "lat", "depth", None),
        P("lat", "depth", None),
        P("lat", "depth", None),
        P(),
        P(),
        P(),
    )
    out_specs = (
        P(None, "lat", "depth", None),
        P(None, "lat", "depth", None),
        P(None, "lat", "depth", None),
        P("lat", "depth", None),
        P(None, "lat", "depth", None),
        P(None, "lat", "depth", None),
        P(None, "lat", "depth", None),
        P("lat", "depth", None),
    )
    return jax.shard_map(
        on_device, mesh=mesh, in_specs=in_specs, out_specs=out_specs, check_vma=False
    )
```
